256 devices in a mesh: rep: 2 (over y_lo), shard: 128 (over z, x, y_hi, core).
Axes of the slice: x: 4, y: 4 (y_hi: 2, y_lo: 2; y = y_hi * 2 + y_lo), z: 8, core: 2. Of those that a mesh axis runs over, the one named last changes fastest.
Arguments:
- row_ids: int32 [2, 128, 128, 16], P('rep', 'shard'), may hold values from -1 to 1310719, as said below
- grad_rows: bfloat16 [2, 128, 128, 16, 128], P('rep', 'shard'), may hold values from -6 to 6
- touched: int32 [128, 20], P('shard'), may hold values from 0 to 39, as said below
- block_home: int32 [5120], replicated, may hold values from 0 to 5119, as said below
- embed_table: float32 [1310720, 128], P('shard'), may hold values from -4 to 4
- row_accum: float32 [1310720], P('shard'), may hold values from 0.001 to 0.1
Outputs:
- new_table: float32 [1310720, 128], P('shard')
- new_accum: float32 [1310720], P('shard')
The draws below stay inside these ranges and needn't reach their ends.
Inputs may be any that keep to these rules, and one draw needn't show every extreme that they name: block_home is a permutation of 0 to 5119. Each row of touched holds 20 different local block numbers. `row_ids`: A live slot in bucket d of any device names a logical row whose stored row lies on index d of shard, in a local block listed in row d of touched; about three quarters of the slots are live.
All inputs are finite; a program needn't handle non-finite values.
Results may differ from the reference program's by a relative error of at most 0.0003.
Values may be sent and summed in bfloat16 or wider, within the bound.
A program may use at most 64 MiB of HBM per device.

```python
import math
import jax
import jax.numpy as jnp
from jax import lax

E = 128
BLOCK = 256
BLK_DEV = 40
TOUCH = 20
SLOT = 16
BLOCKS = 5120
ROWS = 1310720
N_REP = 2
N_SHARD = 128


def layout_tables(key):
    home_key = jax.random.fold_in(key, 11)
    touch_key = jax.random.fold_in(key, 12)
    home_of = jax.random.permutation(home_key, BLOCKS).astype(jnp.int32)
    shard_keys = jax.random.split(touch_key, N_SHARD)
    listed = jax.vmap(lambda each_key: jax.random.permutation(each_key, BLK_DEV)[:TOUCH])(shard_keys)
    return (home_of, listed.astype(jnp.int32))


def draw_block_home(key, part):
    return layout_tables(key)[0]


def draw_touched(key, part):
    return layout_tables(key)[1]


def draw_row_ids(key, part):
    home_of, listed = layout_tables(key)
    block_of_home = jnp.argsort(home_of, stable=True).astype(jnp.int32)
    base_key = jax.random.fold_in(key, 13)
    pick_key, within_key, live_key = jax.random.split(base_key, 3)
    shape = (N_REP, N_SHARD, N_SHARD, SLOT)
    picked = jax.random.randint(pick_key, shape, 0, TOUCH)
    within = jax.random.randint(within_key, shape, 0, BLOCK)
    is_live = jax.random.randint(live_key, shape, 0, 4) < 3
    target = jax.lax.broadcasted_iota(jnp.int32, shape, 2)
    local_block = listed[target, picked]
    logical = block_of_home[target * BLK_DEV + local_block]
    return jnp.where(is_live, logical * BLOCK + within, -1).astype(jnp.int32)


def draw_grad_rows(key, part):
    slot_ids = draw_row_ids(key, part)
    noise_key = jax.random.fold_in(key, 14)
    common_key = jax.random.fold_in(key, 15)
    shape = (N_REP, N_SHARD, N_SHARD, SLOT, E)
    safe_ids = jnp.maximum(slot_ids, 0).reshape(-1)
    shared = jax.vmap(lambda each_id: jax.random.normal(jax.random.fold_in(common_key, each_id), (E,), jnp.float32))(safe_ids)
    shared = jnp.clip(shared, -6.0, 6.0).reshape(shape)
    noise = jnp.clip(jax.random.normal(noise_key, shape, jnp.float32), -6.0, 6.0)
    weight_shared = 0.6
    return jnp.clip(noise + weight_shared * shared, -6.0, 6.0).astype(jnp.bfloat16)


def steps_of(own_key, extent, cuts, smallest, top_value):
    loudness = 1.0
    for dim, shards_of in cuts:
        heights = jax.random.uniform(jax.random.fold_in(jax.random.fold_in(own_key, 6), dim), (shards_of,), jnp.float32, smallest / len(cuts), top_value / len(cuts))
        loudness = loudness * jnp.repeat(jnp.exp(heights), extent[dim] // shards_of).reshape((-1,) + (1,) * (len(extent) - 1 - dim))
    return loudness


def centred(key, dims, deviation, most, cuts=(), kind=jnp.bfloat16):
    entries = deviation * jax.random.normal(key, dims, jnp.float32)
    if cuts:
        entries = entries * steps_of(key, dims, cuts, -0.22, 0.18)
    return jnp.clip(entries, -most, most).astype(kind)


def setup_inputs(seed: int = 0) -> dict:
    seeds = jax.random.split(jax.random.key(seed), 7)
    return {
        "row_ids": draw_row_ids(jax.random.fold_in(seeds[6], 71), 0),
        "grad_rows": draw_grad_rows(jax.random.fold_in(seeds[6], 71), 0),
        "touched": draw_touched(jax.random.fold_in(seeds[6], 71), 0),
        "block_home": draw_block_home(jax.random.fold_in(seeds[6], 71), 0),
        "embed_table": centred(seeds[4], (ROWS, E), 0.5, 4.0, ((0, 128),), jnp.float32),
        "row_accum": jnp.clip(jnp.exp(math.log(0.1) - 4.6051702 * jax.random.uniform(seeds[5], (ROWS,), jnp.float32) ** steps_of(seeds[5], (ROWS,), ((0, 128),), -0.2, 0.2)), 0.001, 0.1),
    }


CLIP_RMS = 0.25
LEARN_RATE = 0.1
DECAY_RATE = 0.05

def reference(row_ids, grad_rows, touched, block_home, embed_table, row_accum):
    sample_ids = row_ids.reshape(-1).astype(jnp.int32)
    gradients = grad_rows.reshape(-1, E).astype(jnp.float32)
    is_live = sample_ids >= 0
    safe_ids = jnp.where(is_live, sample_ids, 0)
    stored = block_home[safe_ids // BLOCK] * BLOCK + safe_ids % BLOCK
    stored = jnp.where(is_live, stored, ROWS).astype(jnp.int32)
    summed = jax.ops.segment_sum(gradients, stored, num_segments=ROWS + 1)[:ROWS]
    square_sum = jnp.sum(summed * summed)
    clip_limit = CLIP_RMS * (N_SHARD * TOUCH * BLOCK * E) ** 0.5
    clip_factor = clip_limit / jnp.maximum(jnp.sqrt(square_sum), clip_limit)
    scaled = summed * clip_factor
    new_accum = row_accum + lax.optimization_barrier(jnp.mean(scaled * scaled, axis=1))
    owners = jnp.arange(N_SHARD, dtype=jnp.int32)[:, None] * BLK_DEV
    touched_blocks = (owners + touched.astype(jnp.int32)).reshape(-1)
    block_mask = jnp.zeros((BLOCKS,), jnp.float32).at[touched_blocks].set(1.0)
    row_mask = jnp.repeat(block_mask, BLOCK)[:, None]
    decayed = embed_table * (1.0 - DECAY_RATE * row_mask)
    new_table = decayed - LEARN_RATE * scaled / jnp.sqrt(new_accum)[:, None]
    return (new_table, new_accum)
```

```python
import functools
import math

import jax
import jax.numpy as jnp
from jax import lax
from jax.experimental import pallas as pl
from jax.experimental.pallas import tpu as pltpu
from jax.sharding import PartitionSpec as P

MESH = pl.DeviceIdType.MESH
BLOCK = 256
PLANE = 16
CLIP_RMS = 0.25
LEARN_RATE = 0.1
DECAY_RATE = 0.05


def key_kernel(blocks_here, ids_ref, home_ref, code_ref):
    ids = ids_ref[...]
    slots, dests = ids.shape
    live = ids >= 0
    safe = jnp.where(live, ids, 0)
    logical = safe >> 8
    high, low = logical >> 7, logical & 127
    stored = jnp.zeros_like(ids)
    for h in range(home_ref.shape[0]):
        row = jnp.broadcast_to(home_ref[h : h + 1, :], ids.shape)
        stored = jnp.where(high == h, jnp.take_along_axis(row, low, axis=1), stored)
    owner = lax.broadcasted_iota(jnp.int32, ids.shape, 1)
    local = stored - owner * blocks_here
    code = jnp.where(live, local * BLOCK + (safe & (BLOCK - 1)), -1)
    padded = jnp.concatenate([code, jnp.zeros((128 - slots, dests), jnp.int32)], axis=0)
    code_ref[...] = padded.T


def exchange_kernel(
    clip_limit,
    grads_hbm,
    codes_ref,
    touched_ref,
    sums_ref,
    clip_ref,
    staged,
    held,
    codes,
    red,
    stage_sem,
    self_sem,
    grad_send,
    grad_recv,
    code_send,
    code_recv,
    pass_send,
    pass_recv,
    passc_send,
    passc_recv,
    red_send,
    red_recv,
):
    rep, me = lax.axis_index("rep"), lax.axis_index("shard")
    shards = held.shape[1]
    planes = shards // PLANE
    z, w = me // PLANE, me % PLANE
    group = (rep + (me // 2) % 2) % 2
    partner = (1 - rep, me)

    def peer_of(d):
        return ((group + (d // 2) % 2) % 2, d)

    stage = pltpu.make_async_copy(grads_hbm, staged, stage_sem)
    stage.start()

    barrier = pltpu.get_barrier_semaphore()
    pl.semaphore_signal(barrier, inc=1, device_id=partner, device_id_type=MESH)

    def greet(i, carry):
        d = (me + i) % shards
        pl.semaphore_signal(barrier, inc=1, device_id=peer_of(d), device_id_type=MESH)
        return carry

    lax.fori_loop(1, shards, greet, 0)
    stage.wait()
    pl.semaphore_wait(barrier, shards)

    def send(d):
        pltpu.make_async_remote_copy(
            src_ref=staged.at[d],
            dst_ref=held.at[group, me],
            send_sem=grad_send,
            recv_sem=grad_recv.at[z],
            device_id=peer_of(d),
            device_id_type=MESH,
        ).start()
        pltpu.make_async_remote_copy(
            src_ref=codes_ref.at[d],
            dst_ref=codes.at[group, me],
            send_sem=code_send,
            recv_sem=code_recv.at[z],
            device_id=peer_of(d),
            device_id_type=MESH,
        ).start()

    own = pltpu.make_async_copy(grads_hbm.at[me], held.at[group, me], self_sem)
    own.start()
    codes[group, me] = codes_ref[me]

    def near(i, carry):
        send(z * PLANE + (w + i) % PLANE)
        return carry

    lax.fori_loop(1, PLANE, near, 0)
    rels = []
    for far in range(planes // 2, 0, -1):
        rels.append([far] if 2 * far == planes else [far, planes - far])
    for pair in rels:

        def farther(i, carry):
            for rel in pair:
                send(((z + rel) % planes) * PLANE + (w + i) % PLANE)
            return carry

        lax.fori_loop(0, PLANE, farther, 0)
    own.wait()

    def chunk(ref, g, zs, count=PLANE):
        return ref.at[g, pl.ds(zs * PLANE, count)]

    def pass_on(zs):
        return (
            pltpu.make_async_remote_copy(
                src_ref=chunk(held, group, zs),
                dst_ref=chunk(held, group, zs),
                send_sem=pass_send,
                recv_sem=pass_recv.at[zs],
                device_id=partner,
                device_id_type=MESH,
            ),
            pltpu.make_async_remote_copy(
                src_ref=chunk(codes, group, zs),
                dst_ref=chunk(codes, group, zs),
                send_sem=passc_send,
                recv_sem=passc_recv.at[zs],
                device_id=partner,
                device_id_type=MESH,
            ),
        )

    def take(rel):
        zs = (z + rel) % planes
        if rel == 0:
            lands = held.at[group, pl.ds(0, PLANE - 1)]
            landc = codes.at[group, pl.ds(0, PLANE - 1)]
        else:
            lands, landc = chunk(held, group, zs), chunk(codes, group, zs)
        pltpu.make_async_copy(lands, lands, grad_recv.at[zs]).wait()
        pltpu.make_async_copy(landc, landc, code_recv.at[zs]).wait()
        for copy in pass_on(zs):
            copy.start()

    slots = staged.shape[1]
    rows = PLANE * slots
    width = staged.shape[2]
    touch_count = sums_ref.shape[0]
    ones = jnp.ones((width, width), jnp.bfloat16)

    def add(rel, first):
        zs = (z + rel) % planes
        other = 1 - group
        lands, landc = chunk(held, other, zs), chunk(codes, other, zs)
        pltpu.make_async_copy(lands, lands, pass_recv.at[zs]).wait()
        pltpu.make_async_copy(landc, landc, passc_recv.at[zs]).wait()
        grads, blocks, offsets = [], [], []
        lane = lax.broadcasted_iota(jnp.int32, (rows, width), 1)
        slot = lax.broadcasted_iota(jnp.int32, (rows, width), 0) % slots
        for g in range(2):
            grads.append(held[g, pl.ds(zs * PLANE, PLANE)].reshape(rows, width))
            code = jnp.broadcast_to(
                codes[g, pl.ds(zs * PLANE, PLANE)], (PLANE, slots, width)
            ).reshape(rows, width)
            block = jnp.where(lane == slot, code >> 8, 0).astype(jnp.float32)
            offset = jnp.where(lane == slot, code & (BLOCK - 1), 0).astype(jnp.float32)
            blocks.append(block.astype(jnp.bfloat16))
            offsets.append(offset.astype(jnp.bfloat16))
        values = jnp.concatenate(grads, axis=0)
        block = jnp.dot(
            jnp.concatenate(blocks, axis=0), ones, preferred_element_type=jnp.float32
        ).astype(jnp.bfloat16)
        offset = lax.dot_general(
            ones[:16],
            jnp.concatenate(offsets, axis=0),
            (((1,), (1,)), ((), ())),
            preferred_element_type=jnp.float32,
        )
        target = lax.broadcasted_iota(jnp.int32, (BLOCK, 2 * rows), 0).astype(jnp.float32)
        onehot = jnp.where(jnp.broadcast_to(offset[:1], target.shape) == target, 1.0, 0.0)
        onehot = onehot.astype(jnp.bfloat16)
        for pair in range(touch_count // 2):
            picked = []
            for t in (2 * pair, 2 * pair + 1):
                wanted = touched_ref[0, t].astype(jnp.float32).astype(jnp.bfloat16)
                picked.append(jnp.where(block == wanted, values, jnp.bfloat16(0)))
            part = jnp.dot(
                onehot, jnp.concatenate(picked, axis=1), preferred_element_type=jnp.float32
            )
            for k in range(2):
                piece = part[:, k * width : (k + 1) * width]
                if first:
                    sums_ref[2 * pair + k] = piece
                else:
                    sums_ref[2 * pair + k] += piece

    order = [0]
    for pair in rels:
        order += pair
    take(order[0])
    for i, rel in enumerate(order):
        if i + 1 < planes:
            take(order[i + 1])
        add(rel, i == 0)

    def square(t, acc):
        v = sums_ref[t]
        return acc + jnp.sum((v * v).reshape(BLOCK // 8, 8, width), axis=0)

    part = lax.fori_loop(0, touch_count, square, jnp.zeros((8, width), jnp.float32))
    red[me] = jnp.sum(part, axis=0, keepdims=True)

    def tell(i, carry):
        d = (me + i) % shards
        pltpu.make_async_remote_copy(
            src_ref=red.at[me],
            dst_ref=red.at[me],
            send_sem=red_send,
            recv_sem=red_recv,
            device_id=peer_of(d),
            device_id_type=MESH,
        ).start()
        return carry

    lax.fori_loop(1, shards, tell, 0)
    rest = red.at[pl.ds(0, shards - 1)]
    pltpu.make_async_copy(rest, rest, red_recv).wait()
    total = jnp.sum(jnp.sum(red[...], axis=0), axis=1, keepdims=True)
    clip = clip_limit / jnp.maximum(jnp.sqrt(total), clip_limit)
    clip_ref[...] = jnp.broadcast_to(clip, clip_ref.shape)

    pltpu.make_async_copy(rest, rest, red_send).wait()
    sent = staged.at[pl.ds(0, shards - 1)]
    pltpu.make_async_copy(sent, sent, grad_send).wait()
    sentc = codes.at[0, pl.ds(0, shards - 1)]
    pltpu.make_async_copy(sentc, sentc, code_send).wait()
    pltpu.make_async_copy(held.at[0], held.at[0], pass_send).wait()
    pltpu.make_async_copy(codes.at[0], codes.at[0], passc_send).wait()


def update_kernel(per_step, touched_ref, sums_ref, clip_ref, table_ref, accum_ref, out_ref, next_ref, place):
    step = pl.program_id(0)
    touch_count = sums_ref.shape[0]
    width = sums_ref.shape[2]
    halves = BLOCK // width

    @pl.when(step == 0)
    def _():
        for b in range(place.shape[0]):
            place[b] = -1
        for t in range(touch_count):
            place[touched_ref[0, t]] = t

    clip = clip_ref[...]
    diagonal = lax.broadcasted_iota(jnp.int32, (width, width), 0) == lax.broadcasted_iota(
        jnp.int32, (width, width), 1
    )
    for j in range(per_step):
        where = place[step * per_step + j]
        span = pl.ds(j * BLOCK, BLOCK)

        @pl.when(where < 0)
        def _():
            out_ref[span, :] = table_ref[span, :]
            next_ref[j] = accum_ref[j]

        @pl.when(where >= 0)
        def _():
            for h in range(halves):
                part = pl.ds(h * width, width)
                rows = pl.ds(j * BLOCK + h * width, width)
                scaled = sums_ref[where, part, :] * clip
                mean = jnp.sum(scaled * scaled, axis=1, keepdims=True) * (1.0 / width)
                old = accum_ref[j, h : h + 1, :]
                column = jnp.sum(
                    jnp.where(diagonal, jnp.broadcast_to(old, (width, width)), 0.0),
                    axis=1,
                    keepdims=True,
                )
                out_ref[rows, :] = table_ref[rows, :] * (1.0 - DECAY_RATE) - LEARN_RATE * (
                    scaled / jnp.sqrt(column + mean)
                )
                next_ref[j, h : h + 1, :] = old + jnp.sum(
                    jnp.where(diagonal, jnp.broadcast_to(mean, (width, width)), 0.0),
                    axis=0,
                    keepdims=True,
                )


def body(row_ids, grad_rows, touched, block_home, embed_table, row_accum):
    shards, slots, width = grad_rows.shape[2:]
    table_rows = embed_table.shape[0]
    blocks_here = table_rows // BLOCK
    touch_count = touched.shape[1]
    vmem = pl.BlockSpec(memory_space=pltpu.VMEM)
    smem = pl.BlockSpec(memory_space=pltpu.SMEM)

    codes = pl.pallas_call(
        functools.partial(key_kernel, blocks_here),
        out_shape=jax.ShapeDtypeStruct((shards, 128), jnp.int32),
        in_specs=[vmem, vmem],
        out_specs=vmem,
    )(row_ids.reshape(shards, slots).T, block_home.reshape(-1, 128))

    clip_limit = CLIP_RMS * math.sqrt(shards * touch_count * BLOCK * width)
    dma = pltpu.SemaphoreType.DMA
    planes = shards // PLANE
    sums, clip = pl.pallas_call(
        functools.partial(exchange_kernel, clip_limit),
        out_shape=(
            jax.ShapeDtypeStruct((touch_count, BLOCK, width), jnp.float32),
            jax.ShapeDtypeStruct((1, width), jnp.float32),
        ),
        in_specs=[pl.BlockSpec(memory_space=pl.ANY), vmem, smem],
        out_specs=(vmem, vmem),
        scratch_shapes=[
            pltpu.VMEM((shards, slots, width), jnp.bfloat16),
            pltpu.VMEM((2, shards, slots, width), jnp.bfloat16),
            pltpu.VMEM((2, shards, 1, 128), jnp.int32),
            pltpu.VMEM((shards, 1, width), jnp.float32),
            dma,
            dma,
            dma,
            dma((planes,)),
            dma,
            dma((planes,)),
            dma,
            dma((planes,)),
            dma,
            dma((planes,)),
            dma,
            dma,
        ],
        compiler_params=pltpu.CompilerParams(
            collective_id=0, has_side_effects=True, vmem_limit_bytes=32 * 1024 * 1024
        ),
    )(grad_rows.reshape(shards, slots, width), codes.reshape(shards, 1, 128), touched)

    per_step = 5
    steps = blocks_here // per_step
    halves = BLOCK // width
    table, accum = pl.pallas_call(
        functools.partial(update_kernel, per_step),
        grid=(steps,),
        out_shape=(
            jax.ShapeDtypeStruct(embed_table.shape, jnp.float32),
            jax.ShapeDtypeStruct((blocks_here, halves, width), jnp.float32),
        ),
        in_specs=[
            smem,
            vmem,
            vmem,
            pl.BlockSpec((per_step * BLOCK, width), lambda i: (i, 0)),
            pl.BlockSpec((per_step, halves, width), lambda i: (i, 0, 0)),
        ],
        out_specs=(
            pl.BlockSpec((per_step * BLOCK, width), lambda i: (i, 0)),
            pl.BlockSpec((per_step, halves, width), lambda i: (i, 0, 0)),
        ),
        scratch_shapes=[pltpu.SMEM((blocks_here,), jnp.int32)],
        compiler_params=pltpu.CompilerParams(vmem_limit_bytes=24 * 1024 * 1024),
    )(touched, sums, clip, embed_table, row_accum.reshape(blocks_here, halves, width))
    return table, accum.reshape(-1)


def solution(mesh):
    placed = (
        P("rep", "shard", None, None),
        P("rep", "shard", None, None, None),
        P("shard", None),
        P(),
        P("shard", None),
        P("shard"),
    )
    return jax.shard_map(
        body, mesh=mesh, in_specs=placed, out_specs=(P("shard", None), P("shard")), check_vma=False
    )
```

```python
import functools
import math

import jax
import jax.numpy as jnp
from jax import lax
from jax.experimental import pallas as pl
from jax.experimental.pallas import tpu as pltpu
from jax.sharding import PartitionSpec as P

MESH = pl.DeviceIdType.MESH
BLOCK = 256
PLANE = 16
CLIP_RMS = 0.25
LEARN_RATE = 0.1
DECAY_RATE = 0.05


def slot_codes(ids, home_ref, blocks_here, planes):
    slots, dests = ids.shape
    live = ids >= 0
    safe = jnp.where(live, ids, 0)
    logical = safe >> 8
    high, low = logical >> 7, logical & 127
    stored = jnp.zeros_like(ids)
    for h in range(home_ref.shape[0]):
        row = jnp.broadcast_to(home_ref[h : h + 1, :], ids.shape)
        stored = jnp.where(high == h, jnp.take_along_axis(row, low, axis=1), stored)
    owner = lax.broadcasted_iota(jnp.int32, ids.shape, 1)
    local = stored - owner * blocks_here
    code = jnp.where(live, local * BLOCK + (safe & (BLOCK - 1)), -1)
    turned = [code] + [pltpu.roll(code, dests - PLANE * p, 1) for p in range(1, planes)]
    return jnp.concatenate(turned, axis=0).T[:PLANE]


def by_plane(raw, planes):
    sources, lanes = raw.shape
    slots = lanes // planes
    per_row = lanes // slots
    turned = [raw] + [pltpu.roll(raw, slots * m, 1) for m in range(1, per_row)]
    part = lax.broadcasted_iota(jnp.int32, raw.shape, 1) // slots
    source = lax.broadcasted_iota(jnp.int32, raw.shape, 0) % per_row
    found = []
    for p in range(planes):
        picked = jnp.zeros_like(raw)
        for j in range(per_row):
            picked = jnp.where((part == j) & (source == j), turned[(j - p) % per_row], picked)
        found.append(jnp.sum(picked.reshape(sources // per_row, per_row, lanes), axis=1))
    return found


def exchange_kernel(
    clip_limit,
    blocks_here,
    grads_hbm,
    ids_hbm,
    home_hbm,
    touched_hbm,
    sums_ref,
    means_ref,
    clip_ref,
    staged,
    relay,
    held,
    mine,
    raw,
    packed,
    codes,
    ids_ref,
    home_ref,
    touched_ref,
    red_plane,
    red_column,
    load_sem,
    direct_send,
    direct_recv,
    spread_send,
    spread_recv,
    relay_send,
    relay_recv,
    column_send,
    column_recv,
    pass_send,
    pass_recv,
    code_send,
    code_recv,
    ccode_send,
    ccode_recv,
    pcode_send,
    pcode_recv,
    redp_send,
    redp_recv,
    redc_send,
    redc_recv,
):
    rep, me = lax.axis_index("rep"), lax.axis_index("shard")
    shards, slots, width = staged.shape
    planes = shards // PLANE
    z, w = me // PLANE, me % PLANE
    group = (rep + (w // 2) % 2) % 2
    other = 1 - group
    partner = (1 - rep, me)
    mates = [(w + i) % PLANE for i in range(PLANE)]
    mate_ids = [((group + (to // 2) % 2) % 2, z * PLANE + to) for to in mates]

    def ahead(rel):
        return (z + rel) % planes

    def behind(rel):
        return (z + planes - rel) % planes

    def at_column(to):
        return (rep, to * PLANE + w)

    def remote(src, dst, send, recv, device):
        return pltpu.make_async_remote_copy(
            src_ref=src, dst_ref=dst, send_sem=send, recv_sem=recv, device_id=device, device_id_type=MESH
        )

    def wait(ref, sem):
        pltpu.make_async_copy(ref, ref, sem).wait()

    def chunk(ref, g, zs, count=PLANE):
        return ref.at[g, pl.ds(zs * PLANE, count)]

    barrier = pltpu.get_barrier_semaphore()
    for rel in range(planes - 1, 0, -1):
        pl.semaphore_signal(barrier, inc=1, device_id=at_column(ahead(rel)), device_id_type=MESH)
    for i in range(1, PLANE):
        pl.semaphore_signal(barrier, inc=1, device_id=mate_ids[i], device_id_type=MESH)
    pl.semaphore_signal(barrier, inc=1, device_id=partner, device_id_type=MESH)

    loads = [
        pltpu.make_async_copy(ids_hbm, ids_ref, load_sem.at[0]),
        pltpu.make_async_copy(home_hbm, home_ref, load_sem.at[1]),
        pltpu.make_async_copy(grads_hbm, staged, load_sem.at[2]),
        pltpu.make_async_copy(touched_hbm, touched_ref, load_sem.at[3]),
    ]
    for load in loads:
        load.start()

    near = []
    for rel in range(1, planes // 2 - 1):
        near += [rel, planes - rel]
    far = [planes // 2 - 1, planes // 2 + 1, planes // 2]

    for rel in [0] + far:
        to = ahead(rel)
        src = grads_hbm.at[to * PLANE + w]
        dst = held.at[group, me] if rel == 0 else relay.at[to, w]
        pltpu.make_async_copy(src, dst, relay_recv.at[to]).start()

    loads[0].wait()
    loads[1].wait()
    mine[...] = slot_codes(ids_ref[...], home_ref, blocks_here, planes).reshape(mine.shape)
    raw[w] = mine[w]
    loads[2].wait()
    loads[3].wait()
    pl.semaphore_wait(barrier, PLANE + planes - 1)

    for rel in near:
        to = ahead(rel)
        remote(
            staged.at[pl.ds(to * PLANE, PLANE)], relay.at[z], direct_send, direct_recv.at[z], at_column(to)
        ).start()
    for i in range(1, PLANE):
        remote(mine.at[mates[i]], raw.at[w], code_send, code_recv, mate_ids[i]).start()
    for rel in [0] + far:
        to = ahead(rel)
        for i in range(1, PLANE):
            dst = held.at[group, me] if rel == 0 else relay.at[to, w]
            remote(staged.at[to * PLANE + mates[i]], dst, relay_send, relay_recv.at[to], mate_ids[i]).start()

    wait(raw.at[pl.ds(0, PLANE - 1)], code_recv)
    for p, rows in enumerate(by_plane(raw[...].reshape(PLANE, planes * slots), planes)):
        packed[p] = rows
    codes[group, z] = packed[z]
    for rel in near + far:
        to = ahead(rel)
        remote(packed.at[to], codes.at[group, z], ccode_send, ccode_recv, at_column(to)).start()

    def send_column(rel):
        to = ahead(rel)
        wait(relay.at[to], relay_recv.at[to])
        remote(
            relay.at[to], chunk(held, group, z), column_send, column_recv.at[z], at_column(to)
        ).start()

    def spread(rel):
        zs = behind(rel)
        wait(relay.at[zs], direct_recv.at[zs])
        place = held.at[group, zs * PLANE + w]
        for i in range(1, PLANE):
            remote(relay.at[zs, mates[i]], place, spread_send, spread_recv.at[zs], mate_ids[i]).start()
        held[group, zs * PLANE + w] = relay[zs, w]

    def take(rel):
        zs = behind(rel)
        if rel == 0:
            wait(chunk(held, group, zs), relay_recv.at[zs])
        elif rel in near:
            wait(chunk(held, group, 0, PLANE - 1), spread_recv.at[zs])
        else:
            wait(chunk(held, group, zs), column_recv.at[zs])
        remote(
            chunk(held, group, zs), chunk(held, group, zs), pass_send, pass_recv.at[zs], partner
        ).start()

    rows = PLANE * slots
    touch_count = sums_ref.shape[0]
    ones = jnp.ones((width, width), jnp.bfloat16)
    diagonal = lax.broadcasted_iota(jnp.int32, (width, width), 0) == lax.broadcasted_iota(
        jnp.int32, (width, width), 1
    )

    def add(rel, first):
        zs = behind(rel)
        wait(chunk(held, other, zs), pass_recv.at[zs])
        grads, blocks, offsets = [], [], []
        for g in range(2):
            grads.append(held[g, pl.ds(zs * PLANE, PLANE)].reshape(rows, width))
            code = codes[g, zs]
            for r in range(rows // width):
                line = code[r : r + 1]
                block = jnp.where(diagonal, jnp.broadcast_to(line >> 8, diagonal.shape), 0)
                blocks.append(block.astype(jnp.float32).astype(jnp.bfloat16))
                offsets.append(line & (BLOCK - 1))
        values = jnp.concatenate(grads, axis=0)
        block = jnp.dot(
            jnp.concatenate(blocks, axis=0), ones, preferred_element_type=jnp.float32
        ).astype(jnp.bfloat16)
        target = lax.broadcasted_iota(jnp.int32, (BLOCK, 2 * rows), 0)
        offset = jnp.broadcast_to(jnp.concatenate(offsets, axis=1), target.shape)
        onehot = jnp.where(offset == target, 1.0, 0.0).astype(jnp.bfloat16)
        for pair in range(touch_count // 2):
            picked = []
            for t in (2 * pair, 2 * pair + 1):
                wanted = touched_ref[0, t].astype(jnp.float32).astype(jnp.bfloat16)
                picked.append(jnp.where(block == wanted, values, jnp.bfloat16(0)))
            part = jnp.dot(
                onehot, jnp.concatenate(picked, axis=1), preferred_element_type=jnp.float32
            )
            for k in range(2):
                piece = part[:, k * width : (k + 1) * width]
                if first:
                    sums_ref[2 * pair + k] = piece
                else:
                    sums_ref[2 * pair + k] += piece

    for rel in far:
        send_column(rel)
    take(0)
    for rel in near:
        spread(rel)
    wait(codes.at[group, pl.ds(0, planes - 1)], ccode_recv)
    remote(codes.at[group], codes.at[group], pcode_send, pcode_recv, partner).start()
    every = [0] + near + far
    take(every[1])
    take(every[2])
    wait(codes.at[other], pcode_recv)
    for i, rel in enumerate(every):
        if i + 3 < planes:
            take(every[i + 3])
        add(rel, i == 0)

    def square(t, acc):
        v = sums_ref[t]
        return acc + jnp.sum((v * v).reshape(BLOCK // 8, 8, width), axis=0)

    part = lax.fori_loop(0, touch_count, square, jnp.zeros((8, width), jnp.float32))
    red_plane[w] = jnp.sum(part, axis=0, keepdims=True)
    for i in range(1, PLANE):
        remote(red_plane.at[w], red_plane.at[w], redp_send, redp_recv, mate_ids[i]).start()

    def row_means(t, carry):
        for h in range(BLOCK // width):
            v = sums_ref[t, pl.ds(h * width, width), :]
            mean = jnp.sum(v * v, axis=1, keepdims=True) * (1.0 / width)
            means_ref[t, h : h + 1, :] = jnp.sum(
                jnp.where(diagonal, jnp.broadcast_to(mean, diagonal.shape), 0.0), axis=0, keepdims=True
            )
        return carry

    lax.fori_loop(0, touch_count, row_means, 0)

    wait(red_plane.at[pl.ds(0, PLANE - 1)], redp_recv)
    red_column[z] = jnp.sum(red_plane[...], axis=0)
    for rel in range(1, planes):
        remote(red_column.at[z], red_column.at[z], redc_send, redc_recv, at_column(ahead(rel))).start()
    wait(red_column.at[pl.ds(0, planes - 1)], redc_recv)
    total = jnp.sum(jnp.sum(red_column[...], axis=0), axis=1, keepdims=True)
    clip = clip_limit / jnp.maximum(jnp.sqrt(total), clip_limit)
    clip_ref[...] = jnp.broadcast_to(clip, clip_ref.shape)

    wait(red_plane.at[pl.ds(0, PLANE - 1)], redp_send)
    wait(red_column.at[pl.ds(0, planes - 1)], redc_send)
    wait(mine.at[pl.ds(0, PLANE - 1)], code_send)
    wait(packed.at[pl.ds(0, planes - 1)], ccode_send)
    wait(codes.at[0], pcode_send)
    wait(staged.at[pl.ds(0, len(near) * PLANE)], direct_send)
    wait(staged.at[pl.ds(0, len(near) * (PLANE - 1))], spread_send)
    wait(staged.at[pl.ds(0, (len(far) + 1) * (PLANE - 1))], relay_send)
    wait(staged.at[pl.ds(0, len(far) * PLANE)], column_send)
    wait(held.at[0], pass_send)


def update_kernel(
    touched_ref,
    sums_ref,
    means_ref,
    clip_ref,
    table_ref,
    accum_ref,
    out_ref,
    next_ref,
    place,
    fresh,
    following,
    kept_sem,
    fresh_sem,
    next_sem,
):
    touch_count, _, width = sums_ref.shape
    blocks_here = table_ref.shape[0]
    halves = BLOCK // width

    for b in range(blocks_here):
        place[b] = 0
    for t in range(touch_count):
        place[touched_ref[0, t]] = 1
    for b in range(blocks_here):

        @pl.when(place[b] == 0)
        def _():
            pltpu.make_async_copy(table_ref.at[b], out_ref.at[b], kept_sem).start()

    clip = clip_ref[...]
    following[...] = accum_ref[...]
    for t in range(touch_count):
        b = touched_ref[0, t]
        following[b] = accum_ref[b] + clip * clip * means_ref[t]
    done = pltpu.make_async_copy(following, next_ref, next_sem)
    done.start()

    diagonal = lax.broadcasted_iota(jnp.int32, (width, width), 0) == lax.broadcasted_iota(
        jnp.int32, (width, width), 1
    )

    def renew(t, carry):
        b = touched_ref[0, t]
        rate = (LEARN_RATE * clip) / jnp.sqrt(following[b])
        for h in range(halves):
            column = jnp.sum(
                jnp.where(diagonal, jnp.broadcast_to(rate[h : h + 1], diagonal.shape), 0.0),
                axis=1,
                keepdims=True,
            )
            part = pl.ds(h * width, width)
            fresh[t, part, :] = table_ref[b, part, :] * (1.0 - DECAY_RATE) - column * sums_ref[t, part, :]
        pltpu.make_async_copy(fresh.at[t], out_ref.at[b], fresh_sem).start()
        return carry

    lax.fori_loop(0, touch_count, renew, 0)
    kept = table_ref.at[pl.ds(0, blocks_here - touch_count)]
    pltpu.make_async_copy(kept, kept, kept_sem).wait()
    pltpu.make_async_copy(fresh, fresh, fresh_sem).wait()
    done.wait()


def body(row_ids, grad_rows, touched, block_home, embed_table, row_accum):
    shards, slots, width = grad_rows.shape[2:]
    blocks_here = embed_table.shape[0] // BLOCK
    touch_count = touched.shape[1]
    halves = BLOCK // width
    planes = shards // PLANE
    vmem = pl.BlockSpec(memory_space=pltpu.VMEM)
    smem = pl.BlockSpec(memory_space=pltpu.SMEM)
    hbm = pl.BlockSpec(memory_space=pltpu.HBM)
    dma = pltpu.SemaphoreType.DMA
    f32 = jnp.float32

    clip_limit = CLIP_RMS * math.sqrt(shards * touch_count * BLOCK * width)
    homes = block_home.reshape(-1, 128)
    sums, means, clip = pl.pallas_call(
        functools.partial(exchange_kernel, clip_limit, blocks_here),
        out_shape=(
            jax.ShapeDtypeStruct((touch_count, BLOCK, width), f32),
            jax.ShapeDtypeStruct((touch_count, halves, width), f32),
            jax.ShapeDtypeStruct((1, width), f32),
        ),
        in_specs=[hbm] * 4,
        out_specs=(vmem, vmem, vmem),
        scratch_shapes=[
            pltpu.VMEM((shards, slots, width), jnp.bfloat16),
            pltpu.VMEM((planes, PLANE, slots, width), jnp.bfloat16),
            pltpu.VMEM((2, shards, slots, width), jnp.bfloat16),
            pltpu.VMEM((PLANE, 1, 128), jnp.int32),
            pltpu.VMEM((PLANE, 1, 128), jnp.int32),
            pltpu.VMEM((planes, PLANE * slots // 128, 128), jnp.int32),
            pltpu.VMEM((2, planes, PLANE * slots // 128, 128), jnp.int32),
            pltpu.VMEM((slots, shards), jnp.int32),
            pltpu.VMEM(homes.shape, jnp.int32),
            pltpu.SMEM(touched.shape, jnp.int32),
            pltpu.VMEM((PLANE, 1, width), f32),
            pltpu.VMEM((planes, 1, width), f32),
            dma((4,)),
            dma,
            dma((planes,)),
            dma,
            dma((planes,)),
            dma,
            dma((planes,)),
            dma,
            dma((planes,)),
            dma,
            dma((planes,)),
            *([dma] * 10),
        ],
        compiler_params=pltpu.CompilerParams(
            collective_id=0, has_side_effects=True, vmem_limit_bytes=24 * 1024 * 1024
        ),
        cost_estimate=pl.CostEstimate(
            flops=4 * shards * slots * touch_count * BLOCK * width,
            bytes_accessed=2 * shards * slots * width,
            transcendentals=0,
        ),
    )(
        *(
            pltpu.with_memory_space_constraint(x, pltpu.HBM)
            for x in (
                grad_rows.reshape(shards, slots, width),
                row_ids.reshape(shards, slots).T,
                homes,
                touched,
            )
        )
    )

    table, accum = pl.pallas_call(
        update_kernel,
        out_shape=(
            jax.ShapeDtypeStruct((blocks_here, BLOCK, width), f32),
            jax.ShapeDtypeStruct((blocks_here, halves, width), f32),
        ),
        in_specs=[smem, vmem, vmem, vmem, vmem, vmem],
        out_specs=(hbm, hbm),
        scratch_shapes=[
            pltpu.SMEM((blocks_here,), jnp.int32),
            pltpu.VMEM((touch_count, BLOCK, width), f32),
            pltpu.VMEM((blocks_here, halves, width), f32),
            dma,
            dma,
            dma,
        ],
        compiler_params=pltpu.CompilerParams(vmem_limit_bytes=24 * 1024 * 1024),
    )(
        touched,
        sums,
        means,
        clip,
        embed_table.reshape(blocks_here, BLOCK, width),
        row_accum.reshape(blocks_here, halves, width),
    )
    return table.reshape(embed_table.shape), accum.reshape(-1)


def solution(mesh):
    placed = (
        P("rep", "shard", None, None),
        P("rep", "shard", None, None, None),
        P("shard", None),
        P(),
        P("shard", None),
        P("shard"),
    )
    return jax.shard_map(
        body, mesh=mesh, in_specs=placed, out_specs=(P("shard", None), P("shard")), check_vma=False
    )
```

```python
import functools
import math

import jax
import jax.numpy as jnp
from jax import lax
from jax.experimental import pallas as pl
from jax.experimental.pallas import tpu as pltpu
from jax.sharding import PartitionSpec as P

MESH = pl.DeviceIdType.MESH
BLOCK = 256
PLANE = 16
CLIP_RMS = 0.25
LEARN_RATE = 0.1
DECAY_RATE = 0.05


def slot_codes(ids, home_ref, blocks_here, planes):
    slots, dests = ids.shape
    live = ids >= 0
    safe = jnp.where(live, ids, 0)
    logical = safe >> 8
    high, low = logical >> 7, logical & 127
    stored = jnp.zeros_like(ids)
    for h in range(home_ref.shape[0]):
        row = jnp.broadcast_to(home_ref[h : h + 1, :], ids.shape)
        stored = jnp.where(high == h, jnp.take_along_axis(row, low, axis=1), stored)
    owner = lax.broadcasted_iota(jnp.int32, ids.shape, 1)
    local = stored - owner * blocks_here
    code = jnp.where(live, local * BLOCK + (safe & (BLOCK - 1)), -1)
    turned = [code] + [pltpu.roll(code, dests - PLANE * p, 1) for p in range(1, planes)]
    return jnp.concatenate(turned, axis=0).T[:PLANE]


def by_plane(raw, planes):
    sources, lanes = raw.shape
    slots = lanes // planes
    per_row = lanes // slots
    turned = [raw] + [pltpu.roll(raw, slots * m, 1) for m in range(1, per_row)]
    part = lax.broadcasted_iota(jnp.int32, raw.shape, 1) // slots
    source = lax.broadcasted_iota(jnp.int32, raw.shape, 0) % per_row
    found = []
    for p in range(planes):
        picked = jnp.zeros_like(raw)
        for j in range(per_row):
            picked = jnp.where((part == j) & (source == j), turned[(j - p) % per_row], picked)
        found.append(jnp.sum(picked.reshape(sources // per_row, per_row, lanes), axis=1))
    return found


def exchange_kernel(
    clip_limit,
    blocks_here,
    grads_hbm,
    ids_hbm,
    home_hbm,
    touched_hbm,
    sums_ref,
    means_ref,
    clip_ref,
    staged,
    relay,
    held,
    mine,
    raw,
    packed,
    codes,
    ids_ref,
    home_ref,
    touched_ref,
    red_plane,
    red_column,
    load_sem,
    beyond_sem,
    direct_send,
    direct_recv,
    spread_send,
    spread_recv,
    relay_send,
    relay_recv,
    column_send,
    column_recv,
    pass_send,
    pass_recv,
    code_send,
    code_recv,
    ccode_send,
    ccode_recv,
    pcode_send,
    pcode_recv,
    redp_send,
    redp_recv,
    redc_send,
    redc_recv,
):
    rep, me = lax.axis_index("rep"), lax.axis_index("shard")
    shards, slots, width = staged.shape
    planes = shards // PLANE
    z, w = me // PLANE, me % PLANE
    group = (rep + (w // 2) % 2) % 2
    other = 1 - group
    partner = (1 - rep, me)
    mates = [(w + i) % PLANE for i in range(PLANE)]
    mate_ids = [((group + (to // 2) % 2) % 2, z * PLANE + to) for to in mates]

    def ahead(rel):
        return (z + rel) % planes

    def behind(rel):
        return (z + planes - rel) % planes

    def at_column(to):
        return (rep, to * PLANE + w)

    def remote(src, dst, send, recv, device):
        return pltpu.make_async_remote_copy(
            src_ref=src, dst_ref=dst, send_sem=send, recv_sem=recv, device_id=device, device_id_type=MESH
        )

    def wait(ref, sem):
        pltpu.make_async_copy(ref, ref, sem).wait()

    def chunk(ref, g, zs, count=PLANE):
        return ref.at[g, pl.ds(zs * PLANE, count)]

    near = []
    for rel in range(1, planes // 2 - 1):
        near += [rel, planes - rel]
    far = [planes // 2 - 1, planes // 2 + 1, planes // 2]

    barrier = pltpu.get_barrier_semaphore()
    for rel in near[::-1]:
        pl.semaphore_signal(barrier, inc=1, device_id=at_column(ahead(rel)), device_id_type=MESH)
    for i in range(1, PLANE):
        pl.semaphore_signal(barrier, inc=1, device_id=mate_ids[i], device_id_type=MESH)
    pl.semaphore_signal(barrier, inc=1, device_id=partner, device_id_type=MESH)

    loads = [
        pltpu.make_async_copy(ids_hbm, ids_ref, load_sem.at[0]),
        pltpu.make_async_copy(home_hbm, home_ref, load_sem.at[1]),
        pltpu.make_async_copy(grads_hbm, staged, load_sem.at[2]),
        pltpu.make_async_copy(touched_hbm, touched_ref, load_sem.at[3]),
    ]
    for load in loads:
        load.start()

    for rel in [0] + far:
        to = ahead(rel)
        src = grads_hbm.at[to * PLANE + w]
        dst = held.at[group, me] if rel == 0 else relay.at[to, w]
        pltpu.make_async_copy(src, dst, relay_recv.at[to]).start()

    loads[0].wait()
    loads[1].wait()
    mine[...] = slot_codes(ids_ref[...], home_ref, blocks_here, planes).reshape(mine.shape)
    raw[w] = mine[w]
    loads[2].wait()
    loads[3].wait()
    pl.semaphore_wait(barrier, PLANE + len(near))
    for rel in near[2:]:
        pl.semaphore_signal(beyond_sem, inc=1, device_id=at_column(ahead(rel)), device_id_type=MESH)

    def send_codes():
        for i in range(1, PLANE):
            remote(mine.at[mates[i]], raw.at[w], code_send, code_recv, mate_ids[i]).start()

    def send_mates(rel):
        to = ahead(rel)
        for i in range(1, PLANE):
            dst = held.at[group, me] if rel == 0 else relay.at[to, w]
            remote(staged.at[to * PLANE + mates[i]], dst, relay_send, relay_recv.at[to], mate_ids[i]).start()

    for rel in near:
        to = ahead(rel)
        remote(
            staged.at[pl.ds(to * PLANE, PLANE)], relay.at[z], direct_send, direct_recv.at[z], at_column(to)
        ).start()
    send_codes()
    send_mates(0)
    for rel in far:
        send_mates(rel)

    wait(raw.at[pl.ds(0, PLANE - 1)], code_recv)
    for p, rows in enumerate(by_plane(raw[...].reshape(PLANE, planes * slots), planes)):
        packed[p] = rows
    codes[group, z] = packed[z]
    pl.semaphore_wait(beyond_sem, 2)
    for rel in near + far:
        to = ahead(rel)
        remote(packed.at[to], codes.at[group, z], ccode_send, ccode_recv, at_column(to)).start()

    half = PLANE // 2

    def send_column(rel):
        to = ahead(rel)
        wait(relay.at[to], relay_recv.at[to])
        if rel != far[-1]:
            remote(
                relay.at[to], chunk(held, group, z), column_send, column_recv.at[0, z], at_column(to)
            ).start()
            return
        for k in range(2):
            remote(
                relay.at[to, pl.ds(k * half, half)],
                held.at[group, pl.ds(z * PLANE + k * half, half)],
                column_send,
                column_recv.at[k, z],
                at_column(to),
            ).start()

    def spread(rel):
        zs = behind(rel)
        wait(relay.at[zs], direct_recv.at[zs])
        place = held.at[group, zs * PLANE + w]
        for i in range(1, PLANE):
            remote(relay.at[zs, mates[i]], place, spread_send, spread_recv.at[zs], mate_ids[i]).start()
        held[group, zs * PLANE + w] = relay[zs, w]

    def take(rel):
        zs = behind(rel)
        if rel == 0:
            wait(chunk(held, group, zs), relay_recv.at[zs])
        elif rel in near:
            wait(chunk(held, group, 0, PLANE - 1), spread_recv.at[zs])
        if rel not in far:
            remote(
                chunk(held, group, zs), chunk(held, group, zs), pass_send, pass_recv.at[zs], partner
            ).start()
            return
        if rel != far[-1]:
            piece = chunk(held, group, zs)
            wait(piece, column_recv.at[0, zs])
            remote(piece, piece, pass_send, pass_recv.at[zs], partner).start()
            return
        for k in range(2):
            piece = held.at[group, pl.ds(zs * PLANE + k * half, half)]
            wait(piece, column_recv.at[k, zs])
            remote(piece, piece, pass_send, pass_recv.at[zs], partner).start()

    rows = PLANE * slots
    touch_count = sums_ref.shape[0]
    ones = jnp.ones((width, width), jnp.bfloat16)
    diagonal = lax.broadcasted_iota(jnp.int32, (width, width), 0) == lax.broadcasted_iota(
        jnp.int32, (width, width), 1
    )

    def add(rel, first, last, squares):
        zs = behind(rel)
        wait(chunk(held, other, zs), pass_recv.at[zs])
        grads, blocks, offsets = [], [], []
        for g in range(2):
            grads.append(held[g, pl.ds(zs * PLANE, PLANE)].reshape(rows, width))
            code = codes[g, zs]
            for r in range(rows // width):
                line = code[r : r + 1]
                block = jnp.where(diagonal, jnp.broadcast_to(line >> 8, diagonal.shape), 0)
                blocks.append(block.astype(jnp.float32).astype(jnp.bfloat16))
                offsets.append(line & (BLOCK - 1))
        values = jnp.concatenate(grads, axis=0)
        block = jnp.dot(
            jnp.concatenate(blocks, axis=0), ones, preferred_element_type=jnp.float32
        ).astype(jnp.bfloat16)
        target = lax.broadcasted_iota(jnp.int32, (BLOCK, 2 * rows), 0)
        offset = jnp.broadcast_to(jnp.concatenate(offsets, axis=1), target.shape)
        onehot = jnp.where(offset == target, 1.0, 0.0).astype(jnp.bfloat16)
        for pair in range(touch_count // 2):
            picked = []
            for t in (2 * pair, 2 * pair + 1):
                wanted = touched_ref[0, t].astype(jnp.float32).astype(jnp.bfloat16)
                picked.append(jnp.where(block == wanted, values, jnp.bfloat16(0)))
            part = jnp.dot(
                onehot, jnp.concatenate(picked, axis=1), preferred_element_type=jnp.float32
            )
            for k in range(2):
                piece = part[:, k * width : (k + 1) * width]
                if not first:
                    piece += sums_ref[2 * pair + k]
                sums_ref[2 * pair + k] = piece
                if last:
                    squares += jnp.sum((piece * piece).reshape(BLOCK // 8, 8, width), axis=0)
        return squares

    for rel in far:
        send_column(rel)
    take(0)
    every = [0] + near + far
    for rel in near:
        spread(rel)
    wait(codes.at[group, pl.ds(0, planes - 1)], ccode_recv)
    remote(codes.at[group], codes.at[group], pcode_send, pcode_recv, partner).start()
    take(every[1])
    take(every[2])
    wait(codes.at[other], pcode_recv)
    part = jnp.zeros((8, width), jnp.float32)
    for i, rel in enumerate(every):
        if i + 3 < planes:
            take(every[i + 3])
        part = add(rel, i == 0, i + 1 == planes, part)

    red_plane[w] = jnp.sum(part, axis=0, keepdims=True)
    for i in range(1, PLANE):
        remote(red_plane.at[w], red_plane.at[w], redp_send, redp_recv, mate_ids[i]).start()

    def row_means(t, carry):
        for h in range(BLOCK // width):
            v = sums_ref[t, pl.ds(h * width, width), :]
            mean = jnp.sum(v * v, axis=1, keepdims=True) * (1.0 / width)
            means_ref[t, h : h + 1, :] = jnp.sum(
                jnp.where(diagonal, jnp.broadcast_to(mean, diagonal.shape), 0.0), axis=0, keepdims=True
            )
        return carry

    lax.fori_loop(0, touch_count, row_means, 0)

    wait(red_plane.at[pl.ds(0, PLANE - 1)], redp_recv)
    red_column[z] = jnp.sum(red_plane[...], axis=0)
    for rel in range(1, planes):
        remote(red_column.at[z], red_column.at[z], redc_send, redc_recv, at_column(ahead(rel))).start()
    wait(red_column.at[pl.ds(0, planes - 1)], redc_recv)
    total = jnp.sum(jnp.sum(red_column[...], axis=0), axis=1, keepdims=True)
    clip = clip_limit / jnp.maximum(jnp.sqrt(total), clip_limit)
    clip_ref[...] = jnp.broadcast_to(clip, clip_ref.shape)

    wait(red_plane.at[pl.ds(0, PLANE - 1)], redp_send)
    wait(red_column.at[pl.ds(0, planes - 1)], redc_send)
    wait(mine.at[pl.ds(0, PLANE - 1)], code_send)
    wait(packed.at[pl.ds(0, planes - 1)], ccode_send)
    wait(codes.at[0], pcode_send)
    wait(staged.at[pl.ds(0, len(near) * PLANE)], direct_send)
    wait(staged.at[pl.ds(0, len(near) * (PLANE - 1))], spread_send)
    wait(staged.at[pl.ds(0, (len(far) + 1) * (PLANE - 1))], relay_send)
    wait(staged.at[pl.ds(0, len(far) * PLANE)], column_send)
    wait(held.at[0], pass_send)


def update_kernel(
    touched_ref,
    sums_ref,
    means_ref,
    clip_ref,
    table_ref,
    accum_ref,
    out_ref,
    next_ref,
    place,
    fresh,
    following,
    kept_sem,
    fresh_sem,
    next_sem,
):
    touch_count, _, width = sums_ref.shape
    blocks_here = table_ref.shape[0]
    halves = BLOCK // width

    for b in range(blocks_here):
        place[b] = 0
    for t in range(touch_count):
        place[touched_ref[0, t]] = 1
    for b in range(blocks_here):

        @pl.when(place[b] == 0)
        def _():
            pltpu.make_async_copy(table_ref.at[b], out_ref.at[b], kept_sem).start()

    clip = clip_ref[...]
    following[...] = accum_ref[...]
    for t in range(touch_count):
        b = touched_ref[0, t]
        following[b] = accum_ref[b] + clip * clip * means_ref[t]
    done = pltpu.make_async_copy(following, next_ref, next_sem)
    done.start()

    diagonal = lax.broadcasted_iota(jnp.int32, (width, width), 0) == lax.broadcasted_iota(
        jnp.int32, (width, width), 1
    )

    def renew(t, carry):
        b = touched_ref[0, t]
        rate = (LEARN_RATE * clip) / jnp.sqrt(following[b])
        for h in range(halves):
            column = jnp.sum(
                jnp.where(diagonal, jnp.broadcast_to(rate[h : h + 1], diagonal.shape), 0.0),
                axis=1,
                keepdims=True,
            )
            part = pl.ds(h * width, width)
            fresh[t, part, :] = table_ref[b, part, :] * (1.0 - DECAY_RATE) - column * sums_ref[t, part, :]
        pltpu.make_async_copy(fresh.at[t], out_ref.at[b], fresh_sem).start()
        return carry

    lax.fori_loop(0, touch_count, renew, 0, unroll=5)
    kept = table_ref.at[pl.ds(0, blocks_here - touch_count)]
    pltpu.make_async_copy(kept, kept, kept_sem).wait()
    pltpu.make_async_copy(fresh, fresh, fresh_sem).wait()
    done.wait()


def body(row_ids, grad_rows, touched, block_home, embed_table, row_accum):
    shards, slots, width = grad_rows.shape[2:]
    blocks_here = embed_table.shape[0] // BLOCK
    touch_count = touched.shape[1]
    halves = BLOCK // width
    planes = shards // PLANE
    vmem = pl.BlockSpec(memory_space=pltpu.VMEM)
    smem = pl.BlockSpec(memory_space=pltpu.SMEM)
    hbm = pl.BlockSpec(memory_space=pltpu.HBM)
    dma = pltpu.SemaphoreType.DMA
    f32 = jnp.float32

    clip_limit = CLIP_RMS * math.sqrt(shards * touch_count * BLOCK * width)
    homes = block_home.reshape(-1, 128)
    sums, means, clip = pl.pallas_call(
        functools.partial(exchange_kernel, clip_limit, blocks_here),
        out_shape=(
            jax.ShapeDtypeStruct((touch_count, BLOCK, width), f32),
            jax.ShapeDtypeStruct((touch_count, halves, width), f32),
            jax.ShapeDtypeStruct((1, width), f32),
        ),
        in_specs=[hbm] * 4,
        out_specs=(vmem, vmem, vmem),
        scratch_shapes=[
            pltpu.VMEM((shards, slots, width), jnp.bfloat16),
            pltpu.VMEM((planes, PLANE, slots, width), jnp.bfloat16),
            pltpu.VMEM((2, shards, slots, width), jnp.bfloat16),
            pltpu.VMEM((PLANE, 1, 128), jnp.int32),
            pltpu.VMEM((PLANE, 1, 128), jnp.int32),
            pltpu.VMEM((planes, PLANE * slots // 128, 128), jnp.int32),
            pltpu.VMEM((2, planes, PLANE * slots // 128, 128), jnp.int32),
            pltpu.VMEM((slots, shards), jnp.int32),
            pltpu.VMEM(homes.shape, jnp.int32),
            pltpu.SMEM(touched.shape, jnp.int32),
            pltpu.VMEM((PLANE, 1, width), f32),
            pltpu.VMEM((planes, 1, width), f32),
            dma((4,)),
            pltpu.SemaphoreType.REGULAR,
            dma,
            dma((planes,)),
            dma,
            dma((planes,)),
            dma,
            dma((planes,)),
            dma,
            dma((2, planes)),
            dma,
            dma((planes,)),
            *([dma] * 10),
        ],
        compiler_params=pltpu.CompilerParams(
            collective_id=0, has_side_effects=True, vmem_limit_bytes=24 * 1024 * 1024
        ),
        cost_estimate=pl.CostEstimate(
            flops=4 * shards * slots * touch_count * BLOCK * width,
            bytes_accessed=2 * shards * slots * width,
            transcendentals=0,
        ),
    )(
        *(
            pltpu.with_memory_space_constraint(x, pltpu.HBM)
            for x in (
                grad_rows.reshape(shards, slots, width),
                row_ids.reshape(shards, slots).T,
                homes,
                touched,
            )
        )
    )

    table, accum = pl.pallas_call(
        update_kernel,
        out_shape=(
            jax.ShapeDtypeStruct((blocks_here, BLOCK, width), f32),
            jax.ShapeDtypeStruct((blocks_here, halves, width), f32),
        ),
        in_specs=[smem, vmem, vmem, vmem, vmem, vmem],
        out_specs=(hbm, hbm),
        scratch_shapes=[
            pltpu.SMEM((blocks_here,), jnp.int32),
            pltpu.VMEM((touch_count, BLOCK, width), f32),
            pltpu.VMEM((blocks_here, halves, width), f32),
            dma,
            dma,
            dma,
        ],
        compiler_params=pltpu.CompilerParams(vmem_limit_bytes=24 * 1024 * 1024),
    )(
        touched,
        sums,
        means,
        clip,
        embed_table.reshape(blocks_here, BLOCK, width),
        row_accum.reshape(blocks_here, halves, width),
    )
    return table.reshape(embed_table.shape), accum.reshape(-1)


def solution(mesh):
    placed = (
        P("rep", "shard", None, None),
        P("rep", "shard", None, None, None),
        P("shard", None),
        P(),
        P("shard", None),
        P("shard"),
    )
    return jax.shard_map(
        body, mesh=mesh, in_specs=placed, out_specs=(P("shard", None), P("shard")), check_vma=False
    )
```

```python
import functools
import math

import jax
import jax.numpy as jnp
from jax import lax
from jax.experimental import pallas as pl
from jax.experimental.pallas import tpu as pltpu
from jax.sharding import PartitionSpec as P

MESH = pl.DeviceIdType.MESH
BLOCK = 256
PLANE = 16
CLIP_RMS = 0.25
LEARN_RATE = 0.1
DECAY_RATE = 0.05


def slot_codes(ids, home_ref, blocks_here, planes):
    slots, dests = ids.shape
    live = ids >= 0
    safe = jnp.where(live, ids, 0)
    logical = safe >> 8
    high, low = logical >> 7, logical & 127
    stored = jnp.zeros_like(ids)
    for h in range(home_ref.shape[0]):
        row = jnp.broadcast_to(home_ref[h : h + 1, :], ids.shape)
        stored = jnp.where(high == h, jnp.take_along_axis(row, low, axis=1), stored)
    owner = lax.broadcasted_iota(jnp.int32, ids.shape, 1)
    local = stored - owner * blocks_here
    code = jnp.where(live, local * BLOCK + (safe & (BLOCK - 1)), -1)
    turned = [code] + [pltpu.roll(code, dests - PLANE * p, 1) for p in range(1, planes)]
    return jnp.concatenate(turned, axis=0).T[:PLANE]


def by_plane(raw, planes):
    sources, lanes = raw.shape
    slots = lanes // planes
    per_row = lanes // slots
    turned = [raw] + [pltpu.roll(raw, slots * m, 1) for m in range(1, per_row)]
    part = lax.broadcasted_iota(jnp.int32, raw.shape, 1) // slots
    source = lax.broadcasted_iota(jnp.int32, raw.shape, 0) % per_row
    found = []
    for p in range(planes):
        picked = jnp.zeros_like(raw)
        for j in range(per_row):
            picked = jnp.where((part == j) & (source == j), turned[(j - p) % per_row], picked)
        found.append(jnp.sum(picked.reshape(sources // per_row, per_row, lanes), axis=1))
    return found


def exchange_kernel(
    clip_limit,
    blocks_here,
    grads_hbm,
    ids_hbm,
    home_hbm,
    touched_hbm,
    sums_ref,
    means_ref,
    clip_ref,
    staged,
    relay,
    held,
    mine,
    raw,
    packed,
    codes,
    ids_ref,
    home_ref,
    touched_ref,
    red_plane,
    red_column,
    load_sem,
    beyond_sem,
    direct_send,
    direct_recv,
    spread_send,
    spread_recv,
    relay_send,
    relay_recv,
    column_send,
    column_recv,
    pass_send,
    pass_recv,
    code_send,
    code_recv,
    ccode_send,
    ccode_recv,
    pcode_send,
    pcode_recv,
    redp_send,
    redp_recv,
    redc_send,
    redc_recv,
):
    rep, me = lax.axis_index("rep"), lax.axis_index("shard")
    shards, slots, width = staged.shape
    planes = shards // PLANE
    z, w = me // PLANE, me % PLANE
    group = (rep + (w // 2) % 2) % 2
    other = 1 - group
    partner = (1 - rep, me)
    mates = [(w + i) % PLANE for i in range(PLANE)]
    mate_ids = [((group + (to // 2) % 2) % 2, z * PLANE + to) for to in mates]

    def ahead(rel):
        return (z + rel) % planes

    def behind(rel):
        return (z + planes - rel) % planes

    def at_column(to):
        return (rep, to * PLANE + w)

    def remote(src, dst, send, recv, device):
        return pltpu.make_async_remote_copy(
            src_ref=src, dst_ref=dst, send_sem=send, recv_sem=recv, device_id=device, device_id_type=MESH
        )

    def wait(ref, sem):
        pltpu.make_async_copy(ref, ref, sem).wait()

    def chunk(ref, g, zs, count=PLANE):
        return ref.at[g, pl.ds(zs * PLANE, count)]

    near = []
    for rel in range(1, planes // 2 - 1):
        near += [rel, planes - rel]
    far = [planes // 2 - 1, planes // 2 + 1, planes // 2]

    barrier = pltpu.get_barrier_semaphore()
    for rel in near[::-1]:
        pl.semaphore_signal(barrier, inc=1, device_id=at_column(ahead(rel)), device_id_type=MESH)
    for i in range(1, PLANE):
        pl.semaphore_signal(barrier, inc=1, device_id=mate_ids[i], device_id_type=MESH)
    pl.semaphore_signal(barrier, inc=1, device_id=partner, device_id_type=MESH)

    loads = [
        pltpu.make_async_copy(ids_hbm, ids_ref, load_sem.at[0]),
        pltpu.make_async_copy(home_hbm, home_ref, load_sem.at[1]),
        pltpu.make_async_copy(grads_hbm, staged, load_sem.at[2]),
        pltpu.make_async_copy(touched_hbm, touched_ref, load_sem.at[3]),
    ]
    for load in loads:
        load.start()

    for rel in [0] + far:
        to = ahead(rel)
        src = grads_hbm.at[to * PLANE + w]
        dst = held.at[group, me] if rel == 0 else relay.at[to, w]
        pltpu.make_async_copy(src, dst, relay_recv.at[to]).start()

    loads[0].wait()
    loads[1].wait()
    mine[...] = slot_codes(ids_ref[...], home_ref, blocks_here, planes).reshape(mine.shape)
    raw[w] = mine[w]
    loads[2].wait()
    loads[3].wait()
    pl.semaphore_wait(barrier, PLANE + len(near))
    for rel in near[2:]:
        pl.semaphore_signal(beyond_sem, inc=1, device_id=at_column(ahead(rel)), device_id_type=MESH)

    def send_codes():
        for i in range(1, PLANE):
            remote(mine.at[mates[i]], raw.at[w], code_send, code_recv, mate_ids[i]).start()

    def send_mates(rel):
        to = ahead(rel)
        for i in range(1, PLANE):
            dst = held.at[group, me] if rel == 0 else relay.at[to, w]
            remote(staged.at[to * PLANE + mates[i]], dst, relay_send, relay_recv.at[to], mate_ids[i]).start()

    for rel in near:
        to = ahead(rel)
        remote(
            staged.at[pl.ds(to * PLANE, PLANE)], relay.at[z], direct_send, direct_recv.at[z], at_column(to)
        ).start()
    send_codes()
    send_mates(0)
    for rel in far:
        send_mates(rel)

    wait(raw.at[pl.ds(0, PLANE - 1)], code_recv)
    for p, rows in enumerate(by_plane(raw[...].reshape(PLANE, planes * slots), planes)):
        packed[p] = rows
    codes[group, z] = packed[z]
    pl.semaphore_wait(beyond_sem, 2)
    for rel in near + far:
        to = ahead(rel)
        remote(packed.at[to], codes.at[group, z], ccode_send, ccode_recv, at_column(to)).start()

    half = PLANE // 2

    def send_column(rel):
        to = ahead(rel)
        wait(relay.at[to], relay_recv.at[to])
        if rel != far[-1]:
            remote(
                relay.at[to], chunk(held, group, z), column_send, column_recv.at[0, z], at_column(to)
            ).start()
            return
        for k in range(2):
            remote(
                relay.at[to, pl.ds(k * half, half)],
                held.at[group, pl.ds(z * PLANE + k * half, half)],
                column_send,
                column_recv.at[k, z],
                at_column(to),
            ).start()

    def spread(rel):
        zs = behind(rel)
        wait(relay.at[zs], direct_recv.at[zs])
        place = held.at[group, zs * PLANE + w]
        for i in range(1, PLANE):
            remote(relay.at[zs, mates[i]], place, spread_send, spread_recv.at[zs], mate_ids[i]).start()
        held[group, zs * PLANE + w] = relay[zs, w]

    def take(rel):
        zs = behind(rel)
        if rel == 0:
            wait(chunk(held, group, zs), relay_recv.at[zs])
        elif rel in near:
            wait(chunk(held, group, 0, PLANE - 1), spread_recv.at[zs])
        if rel not in far:
            for k in range(4):
                piece = held.at[group, pl.ds(zs * PLANE + k * (PLANE // 4), PLANE // 4)]
                remote(piece, piece, pass_send, pass_recv.at[zs], partner).start()
            return
        if rel != far[-1]:
            piece = chunk(held, group, zs)
            wait(piece, column_recv.at[0, zs])
            remote(piece, piece, pass_send, pass_recv.at[zs], partner).start()
            return
        for k in range(2):
            piece = held.at[group, pl.ds(zs * PLANE + k * half, half)]
            wait(piece, column_recv.at[k, zs])
            remote(piece, piece, pass_send, pass_recv.at[zs], partner).start()

    rows = PLANE * slots
    touch_count = sums_ref.shape[0]
    ones = jnp.ones((width, width), jnp.bfloat16)
    diagonal = lax.broadcasted_iota(jnp.int32, (width, width), 0) == lax.broadcasted_iota(
        jnp.int32, (width, width), 1
    )

    def add(rel, first, last, squares):
        zs = behind(rel)
        wait(chunk(held, other, zs), pass_recv.at[zs])
        grads, blocks, offsets = [], [], []
        for g in range(2):
            grads.append(held[g, pl.ds(zs * PLANE, PLANE)].reshape(rows, width))
            code = codes[g, zs]
            for r in range(rows // width):
                line = code[r : r + 1]
                block = jnp.where(diagonal, jnp.broadcast_to(line >> 8, diagonal.shape), 0)
                blocks.append(block.astype(jnp.float32).astype(jnp.bfloat16))
                offsets.append(line & (BLOCK - 1))
        values = jnp.concatenate(grads, axis=0)
        block = jnp.dot(
            jnp.concatenate(blocks, axis=0), ones, preferred_element_type=jnp.float32
        ).astype(jnp.bfloat16)
        target = lax.broadcasted_iota(jnp.int32, (BLOCK, 2 * rows), 0)
        offset = jnp.broadcast_to(jnp.concatenate(offsets, axis=1), target.shape)
        onehot = jnp.where(offset == target, 1.0, 0.0).astype(jnp.bfloat16)
        for pair in range(touch_count // 2):
            picked = []
            for t in (2 * pair, 2 * pair + 1):
                wanted = touched_ref[0, t].astype(jnp.float32).astype(jnp.bfloat16)
                picked.append(jnp.where(block == wanted, values, jnp.bfloat16(0)))
            part = jnp.dot(
                onehot, jnp.concatenate(picked, axis=1), preferred_element_type=jnp.float32
            )
            for k in range(2):
                piece = part[:, k * width : (k + 1) * width]
                if not first:
                    piece += sums_ref[2 * pair + k]
                sums_ref[2 * pair + k] = piece
                if last:
                    squares += jnp.sum((piece * piece).reshape(BLOCK // 8, 8, width), axis=0)
        return squares

    for rel in far[:-1]:
        send_column(rel)
    take(0)
    every = [0] + near + far
    for rel in near:
        spread(rel)
    send_column(far[-1])
    wait(codes.at[group, pl.ds(0, planes - 1)], ccode_recv)
    remote(codes.at[group], codes.at[group], pcode_send, pcode_recv, partner).start()
    for rel in every[1:5]:
        take(rel)
    wait(codes.at[other], pcode_recv)
    part = jnp.zeros((8, width), jnp.float32)
    for i, rel in enumerate(every):
        if i + 5 < planes:
            take(every[i + 5])
        part = add(rel, i == 0, i + 1 == planes, part)

    red_plane[w] = jnp.sum(part, axis=0, keepdims=True)
    for i in range(1, PLANE):
        remote(red_plane.at[w], red_plane.at[w], redp_send, redp_recv, mate_ids[i]).start()

    def row_means(t, carry):
        for h in range(BLOCK // width):
            v = sums_ref[t, pl.ds(h * width, width), :]
            mean = jnp.sum(v * v, axis=1, keepdims=True) * (1.0 / width)
            means_ref[t, h : h + 1, :] = jnp.sum(
                jnp.where(diagonal, jnp.broadcast_to(mean, diagonal.shape), 0.0), axis=0, keepdims=True
            )
        return carry

    lax.fori_loop(0, touch_count, row_means, 0)

    wait(red_plane.at[pl.ds(0, PLANE - 1)], redp_recv)
    red_column[z] = jnp.sum(red_plane[...], axis=0)
    for rel in range(1, planes):
        remote(red_column.at[z], red_column.at[z], redc_send, redc_recv, at_column(ahead(rel))).start()
    wait(red_column.at[pl.ds(0, planes - 1)], redc_recv)
    total = jnp.sum(jnp.sum(red_column[...], axis=0), axis=1, keepdims=True)
    clip = clip_limit / jnp.maximum(jnp.sqrt(total), clip_limit)
    clip_ref[...] = jnp.broadcast_to(clip, clip_ref.shape)

    wait(red_plane.at[pl.ds(0, PLANE - 1)], redp_send)
    wait(red_column.at[pl.ds(0, planes - 1)], redc_send)
    wait(mine.at[pl.ds(0, PLANE - 1)], code_send)
    wait(packed.at[pl.ds(0, planes - 1)], ccode_send)
    wait(codes.at[0], pcode_send)
    wait(staged.at[pl.ds(0, len(near) * PLANE)], direct_send)
    wait(staged.at[pl.ds(0, len(near) * (PLANE - 1))], spread_send)
    wait(staged.at[pl.ds(0, (len(far) + 1) * (PLANE - 1))], relay_send)
    wait(staged.at[pl.ds(0, len(far) * PLANE)], column_send)
    wait(held.at[0], pass_send)


def update_kernel(
    touched_ref,
    sums_ref,
    means_ref,
    clip_ref,
    table_ref,
    accum_ref,
    out_ref,
    next_ref,
    place,
    fresh,
    following,
    kept_sem,
    fresh_sem,
    next_sem,
):
    touch_count, _, width = sums_ref.shape
    blocks_here = table_ref.shape[0]
    halves = BLOCK // width

    for b in range(blocks_here):
        place[b] = 0
    for t in range(touch_count):
        place[touched_ref[0, t]] = 1
    for b in range(blocks_here):

        @pl.when(place[b] == 0)
        def _():
            pltpu.make_async_copy(table_ref.at[b], out_ref.at[b], kept_sem).start()

    clip = clip_ref[...]
    following[...] = accum_ref[...]
    for t in range(touch_count):
        b = touched_ref[0, t]
        following[b] = accum_ref[b] + clip * clip * means_ref[t]
    done = pltpu.make_async_copy(following, next_ref, next_sem)
    done.start()

    diagonal = lax.broadcasted_iota(jnp.int32, (width, width), 0) == lax.broadcasted_iota(
        jnp.int32, (width, width), 1
    )

    def renew(t, carry):
        b = touched_ref[0, t]
        rate = (LEARN_RATE * clip) / jnp.sqrt(following[b])
        for h in range(halves):
            column = jnp.sum(
                jnp.where(diagonal, jnp.broadcast_to(rate[h : h + 1], diagonal.shape), 0.0),
                axis=1,
                keepdims=True,
            )
            part = pl.ds(h * width, width)
            fresh[t, part, :] = table_ref[b, part, :] * (1.0 - DECAY_RATE) - column * sums_ref[t, part, :]
        pltpu.make_async_copy(fresh.at[t], out_ref.at[b], fresh_sem).start()
        return carry

    lax.fori_loop(0, touch_count, renew, 0, unroll=5)
    kept = table_ref.at[pl.ds(0, blocks_here - touch_count)]
    pltpu.make_async_copy(kept, kept, kept_sem).wait()
    pltpu.make_async_copy(fresh, fresh, fresh_sem).wait()
    done.wait()


def body(row_ids, grad_rows, touched, block_home, embed_table, row_accum):
    shards, slots, width = grad_rows.shape[2:]
    blocks_here = embed_table.shape[0] // BLOCK
    touch_count = touched.shape[1]
    halves = BLOCK // width
    planes = shards // PLANE
    vmem = pl.BlockSpec(memory_space=pltpu.VMEM)
    smem = pl.BlockSpec(memory_space=pltpu.SMEM)
    hbm = pl.BlockSpec(memory_space=pltpu.HBM)
    dma = pltpu.SemaphoreType.DMA
    f32 = jnp.float32

    clip_limit = CLIP_RMS * math.sqrt(shards * touch_count * BLOCK * width)
    homes = block_home.reshape(-1, 128)
    sums, means, clip = pl.pallas_call(
        functools.partial(exchange_kernel, clip_limit, blocks_here),
        out_shape=(
            jax.ShapeDtypeStruct((touch_count, BLOCK, width), f32),
            jax.ShapeDtypeStruct((touch_count, halves, width), f32),
            jax.ShapeDtypeStruct((1, width), f32),
        ),
        in_specs=[hbm] * 4,
        out_specs=(vmem, vmem, vmem),
        scratch_shapes=[
            pltpu.VMEM((shards, slots, width), jnp.bfloat16),
            pltpu.VMEM((planes, PLANE, slots, width), jnp.bfloat16),
            pltpu.VMEM((2, shards, slots, width), jnp.bfloat16),
            pltpu.VMEM((PLANE, 1, 128), jnp.int32),
            pltpu.VMEM((PLANE, 1, 128), jnp.int32),
            pltpu.VMEM((planes, PLANE * slots // 128, 128), jnp.int32),
            pltpu.VMEM((2, planes, PLANE * slots // 128, 128), jnp.int32),
            pltpu.VMEM((slots, shards), jnp.int32),
            pltpu.VMEM(homes.shape, jnp.int32),
            pltpu.SMEM(touched.shape, jnp.int32),
            pltpu.VMEM((PLANE, 1, width), f32),
            pltpu.VMEM((planes, 1, width), f32),
            dma((4,)),
            pltpu.SemaphoreType.REGULAR,
            dma,
            dma((planes,)),
            dma,
            dma((planes,)),
            dma,
            dma((planes,)),
            dma,
            dma((2, planes)),
            dma,
            dma((planes,)),
            *([dma] * 10),
        ],
        compiler_params=pltpu.CompilerParams(
            collective_id=0, has_side_effects=True, vmem_limit_bytes=24 * 1024 * 1024
        ),
        cost_estimate=pl.CostEstimate(
            flops=4 * shards * slots * touch_count * BLOCK * width,
            bytes_accessed=2 * shards * slots * width,
            transcendentals=0,
        ),
    )(
        *(
            pltpu.with_memory_space_constraint(x, pltpu.HBM)
            for x in (
                grad_rows.reshape(shards, slots, width),
                row_ids.reshape(shards, slots).T,
                homes,
                touched,
            )
        )
    )

    table, accum = pl.pallas_call(
        update_kernel,
        out_shape=(
            jax.ShapeDtypeStruct((blocks_here, BLOCK, width), f32),
            jax.ShapeDtypeStruct((blocks_here, halves, width), f32),
        ),
        in_specs=[smem, vmem, vmem, vmem, vmem, vmem],
        out_specs=(hbm, hbm),
        scratch_shapes=[
            pltpu.SMEM((blocks_here,), jnp.int32),
            pltpu.VMEM((touch_count, BLOCK, width), f32),
            pltpu.VMEM((blocks_here, halves, width), f32),
            dma,
            dma,
            dma,
        ],
        compiler_params=pltpu.CompilerParams(vmem_limit_bytes=24 * 1024 * 1024),
    )(
        touched,
        sums,
        means,
        clip,
        embed_table.reshape(blocks_here, BLOCK, width),
        row_accum.reshape(blocks_here, halves, width),
    )
    return table.reshape(embed_table.shape), accum.reshape(-1)


def solution(mesh):
    placed = (
        P("rep", "shard", None, None),
        P("rep", "shard", None, None, None),
        P("shard", None),
        P(),
        P("shard", None),
        P("shard"),
    )
    return jax.shard_map(
        body, mesh=mesh, in_specs=placed, out_specs=(P("shard", None), P("shard")), check_vma=False
    )
```

```python
import functools
import math

import jax
import jax.numpy as jnp
from jax import lax
from jax.experimental import pallas as pl
from jax.experimental.pallas import tpu as pltpu
from jax.sharding import PartitionSpec as P

MESH = pl.DeviceIdType.MESH
BLOCK = 256
PLANE = 16
CLIP_RMS = 0.25
LEARN_RATE = 0.1
DECAY_RATE = 0.05


def slot_codes(ids, home_ref, blocks_here, planes):
    slots, dests = ids.shape
    live = ids >= 0
    safe = jnp.where(live, ids, 0)
    logical = safe >> 8
    high, low = logical >> 7, logical & 127
    stored = jnp.zeros_like(ids)
    for h in range(home_ref.shape[0]):
        row = jnp.broadcast_to(home_ref[h : h + 1, :], ids.shape)
        stored = jnp.where(high == h, jnp.take_along_axis(row, low, axis=1), stored)
    owner = lax.broadcasted_iota(jnp.int32, ids.shape, 1)
    local = stored - owner * blocks_here
    code = jnp.where(live, local * BLOCK + (safe & (BLOCK - 1)), -1)
    turned = [code] + [pltpu.roll(code, dests - PLANE * p, 1) for p in range(1, planes)]
    return jnp.concatenate(turned, axis=0).T[:PLANE]


def by_plane(raw, planes):
    sources, lanes = raw.shape
    slots = lanes // planes
    per_row = lanes // slots
    turned = [raw] + [pltpu.roll(raw, slots * m, 1) for m in range(1, per_row)]
    part = lax.broadcasted_iota(jnp.int32, raw.shape, 1) // slots
    source = lax.broadcasted_iota(jnp.int32, raw.shape, 0) % per_row
    found = []
    for p in range(planes):
        picked = jnp.zeros_like(raw)
        for j in range(per_row):
            picked = jnp.where((part == j) & (source == j), turned[(j - p) % per_row], picked)
        found.append(jnp.sum(picked.reshape(sources // per_row, per_row, lanes), axis=1))
    return found


def exchange_kernel(
    clip_limit,
    blocks_here,
    grads_hbm,
    ids_hbm,
    home_hbm,
    touched_hbm,
    sums_ref,
    means_ref,
    clip_ref,
    staged,
    relay,
    held,
    mine,
    raw,
    packed,
    codes,
    ids_ref,
    home_ref,
    touched_ref,
    red_plane,
    red_column,
    load_sem,
    beyond_sem,
    direct_send,
    direct_recv,
    spread_send,
    spread_recv,
    relay_send,
    relay_recv,
    column_send,
    column_recv,
    pass_send,
    pass_recv,
    code_send,
    code_recv,
    ccode_send,
    ccode_recv,
    pcode_send,
    pcode_recv,
    redp_send,
    redp_recv,
    redc_send,
    redc_recv,
):
    rep, me = lax.axis_index("rep"), lax.axis_index("shard")
    shards, slots, width = staged.shape
    planes = shards // PLANE
    z, w = me // PLANE, me % PLANE
    group = (rep + (w // 2) % 2) % 2
    other = 1 - group
    partner = (1 - rep, me)
    mates = [(w + i) % PLANE for i in range(PLANE)]
    mate_ids = [((group + (to // 2) % 2) % 2, z * PLANE + to) for to in mates]

    def ahead(rel):
        return (z + rel) % planes

    def behind(rel):
        return (z + planes - rel) % planes

    def at_column(to):
        return (rep, to * PLANE + w)

    def remote(src, dst, send, recv, device):
        return pltpu.make_async_remote_copy(
            src_ref=src, dst_ref=dst, send_sem=send, recv_sem=recv, device_id=device, device_id_type=MESH
        )

    def wait(ref, sem):
        pltpu.make_async_copy(ref, ref, sem).wait()

    def chunk(ref, g, zs, count=PLANE):
        return ref.at[g, pl.ds(zs * PLANE, count)]

    near = []
    for rel in range(1, planes // 2 - 1):
        near += [rel, planes - rel]
    far = [planes // 2 - 1, planes // 2 + 1, planes // 2]

    barrier = pltpu.get_barrier_semaphore()
    for rel in near[::-1]:
        pl.semaphore_signal(barrier, inc=1, device_id=at_column(ahead(rel)), device_id_type=MESH)
    for i in range(1, PLANE):
        pl.semaphore_signal(barrier, inc=1, device_id=mate_ids[i], device_id_type=MESH)
    pl.semaphore_signal(barrier, inc=1, device_id=partner, device_id_type=MESH)

    loads = [
        pltpu.make_async_copy(ids_hbm, ids_ref, load_sem.at[0]),
        pltpu.make_async_copy(home_hbm, home_ref, load_sem.at[1]),
        pltpu.make_async_copy(grads_hbm, staged, load_sem.at[2]),
        pltpu.make_async_copy(touched_hbm, touched_ref, load_sem.at[3]),
    ]
    for load in loads:
        load.start()

    for rel in [0] + far:
        to = ahead(rel)
        src = grads_hbm.at[to * PLANE + w]
        dst = held.at[group, me] if rel == 0 else relay.at[to, w]
        pltpu.make_async_copy(src, dst, relay_recv.at[to]).start()

    loads[0].wait()
    loads[1].wait()
    mine[...] = slot_codes(ids_ref[...], home_ref, blocks_here, planes).reshape(mine.shape)
    raw[w] = mine[w]
    loads[2].wait()
    loads[3].wait()
    pl.semaphore_wait(barrier, PLANE + len(near))
    for rel in near[2:]:
        pl.semaphore_signal(beyond_sem, inc=1, device_id=at_column(ahead(rel)), device_id_type=MESH)

    def send_codes():
        for i in range(1, PLANE):
            remote(mine.at[mates[i]], raw.at[w], code_send, code_recv, mate_ids[i]).start()

    def send_mates(rel):
        to = ahead(rel)
        for i in range(1, PLANE):
            dst = held.at[group, me] if rel == 0 else relay.at[to, w]
            remote(staged.at[to * PLANE + mates[i]], dst, relay_send, relay_recv.at[to], mate_ids[i]).start()

    for rel in near:
        to = ahead(rel)
        remote(
            staged.at[pl.ds(to * PLANE, PLANE)], relay.at[z], direct_send, direct_recv.at[z], at_column(to)
        ).start()
    send_codes()
    send_mates(0)
    for rel in far:
        send_mates(rel)

    wait(raw.at[pl.ds(0, PLANE - 1)], code_recv)
    for p, rows in enumerate(by_plane(raw[...].reshape(PLANE, planes * slots), planes)):
        packed[p] = rows
    codes[group, z] = packed[z]
    pl.semaphore_wait(beyond_sem, 2)
    for rel in near + far:
        to = ahead(rel)
        remote(packed.at[to], codes.at[group, z], ccode_send, ccode_recv, at_column(to)).start()

    half = PLANE // 2

    def send_column(rel):
        to = ahead(rel)
        wait(relay.at[to], relay_recv.at[to])
        if rel != far[-1]:
            remote(
                relay.at[to], chunk(held, group, z), column_send, column_recv.at[0, z], at_column(to)
            ).start()
            return
        for k in range(2):
            remote(
                relay.at[to, pl.ds(k * half, half)],
                held.at[group, pl.ds(z * PLANE + k * half, half)],
                column_send,
                column_recv.at[k, z],
                at_column(to),
            ).start()

    def spread(rel):
        zs = behind(rel)
        wait(relay.at[zs], direct_recv.at[zs])
        place = held.at[group, zs * PLANE + w]
        for i in range(1, PLANE):
            remote(relay.at[zs, mates[i]], place, spread_send, spread_recv.at[zs], mate_ids[i]).start()
        held[group, zs * PLANE + w] = relay[zs, w]

    def take(rel):
        zs = behind(rel)
        if rel == 0:
            wait(chunk(held, group, zs), relay_recv.at[zs])
        elif rel in near:
            wait(chunk(held, group, 0, PLANE - 1), spread_recv.at[zs])
        if rel not in far:
            for k in range(4):
                piece = held.at[group, pl.ds(zs * PLANE + k * (PLANE // 4), PLANE // 4)]
                remote(piece, piece, pass_send, pass_recv.at[zs], partner).start()
            return
        if rel != far[-1]:
            piece = chunk(held, group, zs)
            wait(piece, column_recv.at[0, zs])
            remote(piece, piece, pass_send, pass_recv.at[zs], partner).start()
            return
        for k in range(2):
            piece = held.at[group, pl.ds(zs * PLANE + k * half, half)]
            wait(piece, column_recv.at[k, zs])
            remote(piece, piece, pass_send, pass_recv.at[zs], partner).start()

    rows = PLANE * slots
    touch_count = sums_ref.shape[0]
    ones = jnp.ones((width, width), jnp.bfloat16)
    diagonal = lax.broadcasted_iota(jnp.int32, (width, width), 0) == lax.broadcasted_iota(
        jnp.int32, (width, width), 1
    )

    def add(rel, first, last, squares):
        zs = behind(rel)
        wait(chunk(held, other, zs), pass_recv.at[zs])
        grads, blocks, offsets = [], [], []
        for g in range(2):
            grads.append(held[g, pl.ds(zs * PLANE, PLANE)].reshape(rows, width))
            code = codes[g, zs]
            for r in range(rows // width):
                line = code[r : r + 1]
                block = jnp.where(diagonal, jnp.broadcast_to(line >> 8, diagonal.shape), 0)
                blocks.append(block.astype(jnp.float32).astype(jnp.bfloat16))
                offsets.append(line & (BLOCK - 1))
        values = jnp.concatenate(grads, axis=0)
        block = jnp.dot(
            jnp.concatenate(blocks, axis=0), ones, preferred_element_type=jnp.float32
        ).astype(jnp.bfloat16)
        target = lax.broadcasted_iota(jnp.int32, (BLOCK, 2 * rows), 0)
        offset = jnp.broadcast_to(jnp.concatenate(offsets, axis=1), target.shape)
        onehot = jnp.where(offset == target, 1.0, 0.0).astype(jnp.bfloat16)
        for pair in range(touch_count // 2):
            picked = []
            for t in (2 * pair, 2 * pair + 1):
                wanted = touched_ref[0, t].astype(jnp.float32).astype(jnp.bfloat16)
                picked.append(jnp.where(block == wanted, values, jnp.bfloat16(0)))
            part = jnp.dot(
                onehot, jnp.concatenate(picked, axis=1), preferred_element_type=jnp.float32
            )
            for k in range(2):
                piece = part[:, k * width : (k + 1) * width]
                if not first:
                    piece += sums_ref[2 * pair + k]
                sums_ref[2 * pair + k] = piece
                if last:
                    squares += jnp.sum((piece * piece).reshape(BLOCK // 8, 8, width), axis=0)
        return squares

    take(0)
    every = [0] + near + far
    for rel in near[:2]:
        spread(rel)
    for rel in far[:-1]:
        send_column(rel)
    for rel in near[2:]:
        spread(rel)
    send_column(far[-1])
    wait(codes.at[group, pl.ds(0, planes - 1)], ccode_recv)
    remote(codes.at[group], codes.at[group], pcode_send, pcode_recv, partner).start()
    for rel in every[1:5]:
        take(rel)
    wait(codes.at[other], pcode_recv)
    part = jnp.zeros((8, width), jnp.float32)
    for i, rel in enumerate(every):
        if i + 5 < planes:
            take(every[i + 5])
        part = add(rel, i == 0, i + 1 == planes, part)

    red_plane[w] = jnp.sum(part, axis=0, keepdims=True)
    for i in range(1, PLANE):
        remote(red_plane.at[w], red_plane.at[w], redp_send, redp_recv, mate_ids[i]).start()

    def row_means(t, carry):
        for h in range(BLOCK // width):
            v = sums_ref[t, pl.ds(h * width, width), :]
            mean = jnp.sum(v * v, axis=1, keepdims=True) * (1.0 / width)
            means_ref[t, h : h + 1, :] = jnp.sum(
                jnp.where(diagonal, jnp.broadcast_to(mean, diagonal.shape), 0.0), axis=0, keepdims=True
            )
        return carry

    lax.fori_loop(0, touch_count, row_means, 0)

    wait(red_plane.at[pl.ds(0, PLANE - 1)], redp_recv)
    red_column[z] = jnp.sum(red_plane[...], axis=0)
    for rel in range(1, planes):
        remote(red_column.at[z], red_column.at[z], redc_send, redc_recv, at_column(ahead(rel))).start()
    wait(red_column.at[pl.ds(0, planes - 1)], redc_recv)
    total = jnp.sum(jnp.sum(red_column[...], axis=0), axis=1, keepdims=True)
    clip = clip_limit / jnp.maximum(jnp.sqrt(total), clip_limit)
    clip_ref[...] = jnp.broadcast_to(clip, clip_ref.shape)

    wait(red_plane.at[pl.ds(0, PLANE - 1)], redp_send)
    wait(red_column.at[pl.ds(0, planes - 1)], redc_send)
    wait(mine.at[pl.ds(0, PLANE - 1)], code_send)
    wait(packed.at[pl.ds(0, planes - 1)], ccode_send)
    wait(codes.at[0], pcode_send)
    wait(staged.at[pl.ds(0, len(near) * PLANE)], direct_send)
    wait(staged.at[pl.ds(0, len(near) * (PLANE - 1))], spread_send)
    wait(staged.at[pl.ds(0, (len(far) + 1) * (PLANE - 1))], relay_send)
    wait(staged.at[pl.ds(0, len(far) * PLANE)], column_send)
    wait(held.at[0], pass_send)


def update_kernel(
    touched_ref,
    sums_ref,
    means_ref,
    clip_ref,
    table_ref,
    accum_ref,
    out_ref,
    next_ref,
    place,
    fresh,
    following,
    kept_sem,
    fresh_sem,
    next_sem,
):
    touch_count, _, width = sums_ref.shape
    blocks_here = table_ref.shape[0]
    halves = BLOCK // width

    for b in range(blocks_here):
        place[b] = 0
    for t in range(touch_count):
        place[touched_ref[0, t]] = 1
    for b in range(blocks_here):

        @pl.when(place[b] == 0)
        def _():
            pltpu.make_async_copy(table_ref.at[b], out_ref.at[b], kept_sem).start()

    clip = clip_ref[...]
    following[...] = accum_ref[...]
    for t in range(touch_count):
        b = touched_ref[0, t]
        following[b] = accum_ref[b] + clip * clip * means_ref[t]
    done = pltpu.make_async_copy(following, next_ref, next_sem)
    done.start()

    diagonal = lax.broadcasted_iota(jnp.int32, (width, width), 0) == lax.broadcasted_iota(
        jnp.int32, (width, width), 1
    )

    def renew(t, carry):
        b = touched_ref[0, t]
        rate = (LEARN_RATE * clip) / jnp.sqrt(following[b])
        for h in range(halves):
            column = jnp.sum(
                jnp.where(diagonal, jnp.broadcast_to(rate[h : h + 1], diagonal.shape), 0.0),
                axis=1,
                keepdims=True,
            )
            part = pl.ds(h * width, width)
            fresh[t, part, :] = table_ref[b, part, :] * (1.0 - DECAY_RATE) - column * sums_ref[t, part, :]
        pltpu.make_async_copy(fresh.at[t], out_ref.at[b], fresh_sem).start()
        return carry

    lax.fori_loop(0, touch_count, renew, 0, unroll=5)
    kept = table_ref.at[pl.ds(0, blocks_here - touch_count)]
    pltpu.make_async_copy(kept, kept, kept_sem).wait()
    pltpu.make_async_copy(fresh, fresh, fresh_sem).wait()
    done.wait()


def body(row_ids, grad_rows, touched, block_home, embed_table, row_accum):
    shards, slots, width = grad_rows.shape[2:]
    blocks_here = embed_table.shape[0] // BLOCK
    touch_count = touched.shape[1]
    halves = BLOCK // width
    planes = shards // PLANE
    vmem = pl.BlockSpec(memory_space=pltpu.VMEM)
    smem = pl.BlockSpec(memory_space=pltpu.SMEM)
    hbm = pl.BlockSpec(memory_space=pltpu.HBM)
    dma = pltpu.SemaphoreType.DMA
    f32 = jnp.float32

    clip_limit = CLIP_RMS * math.sqrt(shards * touch_count * BLOCK * width)
    homes = block_home.reshape(-1, 128)
    sums, means, clip = pl.pallas_call(
        functools.partial(exchange_kernel, clip_limit, blocks_here),
        out_shape=(
            jax.ShapeDtypeStruct((touch_count, BLOCK, width), f32),
            jax.ShapeDtypeStruct((touch_count, halves, width), f32),
            jax.ShapeDtypeStruct((1, width), f32),
        ),
        in_specs=[hbm] * 4,
        out_specs=(vmem, vmem, vmem),
        scratch_shapes=[
            pltpu.VMEM((shards, slots, width), jnp.bfloat16),
            pltpu.VMEM((planes, PLANE, slots, width), jnp.bfloat16),
            pltpu.VMEM((2, shards, slots, width), jnp.bfloat16),
            pltpu.VMEM((PLANE, 1, 128), jnp.int32),
            pltpu.VMEM((PLANE, 1, 128), jnp.int32),
            pltpu.VMEM((planes, PLANE * slots // 128, 128), jnp.int32),
            pltpu.VMEM((2, planes, PLANE * slots // 128, 128), jnp.int32),
            pltpu.VMEM((slots, shards), jnp.int32),
            pltpu.VMEM(homes.shape, jnp.int32),
            pltpu.SMEM(touched.shape, jnp.int32),
            pltpu.VMEM((PLANE, 1, width), f32),
            pltpu.VMEM((planes, 1, width), f32),
            dma((4,)),
            pltpu.SemaphoreType.REGULAR,
            dma,
            dma((planes,)),
            dma,
            dma((planes,)),
            dma,
            dma((planes,)),
            dma,
            dma((2, planes)),
            dma,
            dma((planes,)),
            *([dma] * 10),
        ],
        compiler_params=pltpu.CompilerParams(
            collective_id=0, has_side_effects=True, vmem_limit_bytes=24 * 1024 * 1024
        ),
        cost_estimate=pl.CostEstimate(
            flops=4 * shards * slots * touch_count * BLOCK * width,
            bytes_accessed=2 * shards * slots * width,
            transcendentals=0,
        ),
    )(
        *(
            pltpu.with_memory_space_constraint(x, pltpu.HBM)
            for x in (
                grad_rows.reshape(shards, slots, width),
                row_ids.reshape(shards, slots).T,
                homes,
                touched,
            )
        )
    )

    table, accum = pl.pallas_call(
        update_kernel,
        out_shape=(
            jax.ShapeDtypeStruct((blocks_here, BLOCK, width), f32),
            jax.ShapeDtypeStruct((blocks_here, halves, width), f32),
        ),
        in_specs=[smem, vmem, vmem, vmem, vmem, vmem],
        out_specs=(hbm, hbm),
        scratch_shapes=[
            pltpu.SMEM((blocks_here,), jnp.int32),
            pltpu.VMEM((touch_count, BLOCK, width), f32),
            pltpu.VMEM((blocks_here, halves, width), f32),
            dma,
            dma,
            dma,
        ],
        compiler_params=pltpu.CompilerParams(vmem_limit_bytes=24 * 1024 * 1024),
    )(
        touched,
        sums,
        means,
        clip,
        embed_table.reshape(blocks_here, BLOCK, width),
        row_accum.reshape(blocks_here, halves, width),
    )
    return table.reshape(embed_table.shape), accum.reshape(-1)


def solution(mesh):
    placed = (
        P("rep", "shard", None, None),
        P("rep", "shard", None, None, None),
        P("shard", None),
        P(),
        P("shard", None),
        P("shard"),
    )
    return jax.shard_map(
        body, mesh=mesh, in_specs=placed, out_specs=(P("shard", None), P("shard")), check_vma=False
    )
```
